32 devices in a mesh: rep: 4 (over x, y), dp: 8 (over z, core).
Axes of the slice: x: 2, y: 2, z: 4, core: 2. Of those that a mesh axis runs over, the one named last changes fastest.
Arguments:
- a: bfloat16 [32, 4, 8192, 896], P(('rep', 'dp')), parts along dimension 0
- g: bfloat16 [32, 4, 8192, 2560], P(('rep', 'dp')), parts along dimension 0
Outputs:
- output: bfloat16 [16, 896, 2560], P('rep'), parts along dimension 0
There are 4 independent parts. The reference program is written for one: setup_inputs(seed, part) draws one part's arguments, and reference() takes and returns one part's arrays. A program takes and returns all parts, laid end to end along the dimension named above; each array names one.
All inputs are finite; a program needn't handle non-finite values.
Results may differ from the reference program's by a relative error of at most 0.012.
Values are sent between devices in bfloat16 or wider.
A program may use at most 2 GiB of HBM per device.

```python
import jax
import jax.numpy as jnp
from jax import lax

DEVICES = 8
MATRICES = 4
TOKENS = 8192
D = 896
FF = 2560


def setup_inputs(seed: int = 0, part: int = 0) -> dict:
    ka, kg, ks = (jax.random.fold_in(k, part) for k in jax.random.split(jax.random.key(seed), 3))
    size = 2.0 ** jax.random.uniform(ks, (DEVICES, MATRICES, 1, 1), jnp.float32, -1.0, 1.0)
    a = jax.random.normal(ka, (DEVICES, MATRICES, TOKENS, D), jnp.float32)
    g = size * jax.random.normal(kg, (DEVICES, MATRICES, TOKENS, FF), jnp.float32) * (DEVICES * TOKENS) ** -0.5
    return {"a": a.astype(jnp.bfloat16), "g": g.astype(jnp.bfloat16)}


def reference(a, g):
    def take(so_far, one):
        return so_far + jnp.einsum("ntd,ntf->ndf", *one, preferred_element_type=jnp.float32), None

    return lax.scan(take, jnp.zeros((MATRICES, D, FF), jnp.float32), (a, g))[0].astype(jnp.bfloat16)
```

```python
import functools

import jax
import jax.numpy as jnp
from jax import lax
from jax.experimental import pallas as pl
from jax.experimental.pallas import tpu as pltpu

COMBINE_LAG = {0: 1, 1: 6, 2: 3, 3: 1}
DELIVER_LAG = {0: 8, 1: 6, 2: 8, 3: 11}
KEEP = {0: 1, 1: 4, 2: 4, 3: 1}
OWN, PAIR_OUT, PAIR_IN, FROM_A, FROM_B, PART, RES = 7, 2, 12, 12, 8, 4, 14
SLICES = 8
PIECES = 2


def kernel(width, a_hbm, g_hbm, out_hbm, a_buf, g_buf, own, pair_out, pair_in, from_a, from_b, part, res,
           a_sem, g_sem, pair_ssem, pair_rsem, a_rsem, b_rsem, part_ssem, res_rsem, left_ssem, right_ssem,
           swap_ssem, store_sem, out_rsem):
    matrices, tokens, rows = a_hbm.shape
    per = g_hbm.shape[2] // width
    chunks = matrices * per
    half = rows // 2
    piece = half // PIECES
    depth = tokens // SLICES

    me = lax.axis_index("dp")
    chip, core = me // 2, me % 2
    place = chip + core * (3 - 2 * chip)
    step_to = 2 - 4 * core
    partner = me + 1 - 2 * core
    up, down = me + step_to, me - step_to

    barrier = pltpu.get_barrier_semaphore()

    def hello(device):
        pl.semaphore_signal(barrier, inc=1, device_id={"dp": device}, device_id_type=pl.DeviceIdType.MESH)

    hello(partner)
    pl.when(place > 0)(lambda: hello(down))
    pl.when(place < 3)(lambda: hello(up))

    def a_load(n, k):
        return pltpu.make_async_copy(
            a_hbm.at[n, pl.ds(k * depth, depth), :], a_buf.at[n % 2, pl.ds(k * depth, depth), :], a_sem.at[n % 2, k])

    def g_load(j):
        return pltpu.make_async_copy(
            g_hbm.at[j // per, :, pl.ds(pl.multiple_of((j % per) * width, width), width)], g_buf.at[j % 2],
            g_sem.at[j % 2])

    for k in range(SLICES):
        a_load(0, k).start()
        if k == 0:
            g_load(0).start()
    pl.semaphore_wait(barrier, 1 + (place > 0).astype(jnp.int32) + (place < 3).astype(jnp.int32))

    def remote(src, dst, ssem, rsem, device):
        return pltpu.make_async_remote_copy(
            src_ref=src, dst_ref=dst, send_sem=ssem, recv_sem=rsem, device_id={"dp": device},
            device_id_type=pl.DeviceIdType.MESH)

    def strip(q):
        return pl.ds(q * piece, piece)

    def pair_copy(j):
        return remote(pair_out.at[j % PAIR_OUT], pair_in.at[j % PAIR_IN], pair_ssem.at[j % PAIR_OUT],
                      pair_rsem.at[j % PAIR_IN], partner)

    def part_copy(j, q, box, rsem, slots, device):
        return remote(part.at[j % PART, strip(q), :], box.at[j % slots, strip(q), :], part_ssem.at[j % PART, q],
                      rsem.at[j % slots, q], device)

    def res_copy(j, q, ssem, device):
        return remote(res.at[j % RES, strip(q), :], res.at[j % RES, strip(q), :], ssem.at[j % RES, q],
                      res_rsem.at[j % RES, q], device)

    def place_of(j, q):
        return out_hbm.at[j // per, pl.ds(pl.multiple_of(core * half + q * piece, 16), piece),
                          pl.ds(pl.multiple_of((j % per) * width, width), width)]

    def swap_copy(j, q):
        return remote(res.at[j % RES, strip(q), :], place_of(j, q), swap_ssem.at[j % RES, q], out_rsem.at[j // per],
                      partner)

    def store_copy(j, q):
        return pltpu.make_async_copy(res.at[j % RES, strip(q), :], place_of(j, q), store_sem.at[j % RES, q])

    def mine(j, q):
        return (own[j % OWN, pl.ds(pl.multiple_of(core * half + q * piece, 16), piece), :]
                + pair_in[j % PAIR_IN, strip(q), :].astype(jnp.float32))

    def outgoing(d, j, q):
        copies = [swap_copy(j, q), store_copy(j, q)]
        if d == 1:
            copies = [res_copy(j, q, right_ssem, up), res_copy(j, q, left_ssem, down)] + copies
        if d == 2:
            copies = [res_copy(j, q, right_ssem, up)] + copies
        return copies

    def finish(d, j):
        for q in range(PIECES):
            outs = outgoing(d, j, q)
            for c in outs[:-1]:
                c.wait_send()
            outs[-1].wait()

    def combine(d, j):
        pair_copy(j).wait_recv()
        for q in range(PIECES):
            total = mine(j, q)
            if d == 2:
                part_copy(j, q, from_a, a_rsem, FROM_A, up).wait_recv()
                total += from_a[j % FROM_A, strip(q), :].astype(jnp.float32)
            if d == 1:
                part_copy(j, q, from_a, a_rsem, FROM_A, down).wait_recv()
                total += from_a[j % FROM_A, strip(q), :].astype(jnp.float32)
                part_copy(j, q, from_b, b_rsem, FROM_B, up).wait_recv()
                total += from_b[j % FROM_B, strip(q), :].astype(jnp.float32)
            if d == 1:
                res[j % RES, strip(q), :] = total.astype(jnp.bfloat16)
                for c in outgoing(1, j, q):
                    c.start()
                continue
            if d == 2:
                copy = functools.partial(part_copy, q=q, box=from_b, rsem=b_rsem, slots=FROM_B, device=down)
            else:
                copy = functools.partial(part_copy, q=q, box=from_a, rsem=a_rsem, slots=FROM_A,
                                         device=up if d == 0 else down)
            pl.when(j >= PART)(lambda: copy(j - PART).wait_send())
            part[j % PART, strip(q), :] = total.astype(jnp.bfloat16)
            copy(j).start()

    def deliver(d, j):
        for q in range(PIECES):
            res_copy(j, q, right_ssem, up).wait_recv()
            for c in outgoing(d, j, q):
                c.start()

    def each_place(f):
        for d in range(4):
            pl.when(place == d)(functools.partial(f, d))

    def step(s, _):
        @pl.when(s < chunks)
        def _():
            n, t = s // per, s % per

            @pl.when(s + 1 < chunks)
            def _():
                g_load(s + 1).start()

            @pl.when((n + 1 < matrices) & (t < SLICES))
            def _():
                a_load(n + 1, t).start()

            @pl.when(t == 0)
            def _():
                for k in range(SLICES):
                    a_load(n, k).wait()

            g_load(s).wait()
            own[s % OWN] = lax.dot_general(
                a_buf[n % 2], g_buf[s % 2], (((0,), (0,)), ((), ())), preferred_element_type=jnp.float32)
            pl.when(s >= PAIR_OUT)(lambda: pair_copy(s - PAIR_OUT).wait_send())
            pair_out[s % PAIR_OUT] = own[
                s % OWN, pl.ds(pl.multiple_of((1 - core) * half, 16), half), :].astype(jnp.bfloat16)
            pair_copy(s).start()

        def stages(d):
            j = s - COMBINE_LAG[d]

            @pl.when((j >= 0) & (j < chunks))
            def _():
                if d == 1:
                    pl.when(j >= KEEP[d])(lambda: finish(d, j - KEEP[d]))
                combine(d, j)

            if d != 1:
                i = s - DELIVER_LAG[d]

                @pl.when((i >= 0) & (i < chunks))
                def _():
                    pl.when(i >= KEEP[d])(lambda: finish(d, i - KEEP[d]))
                    deliver(d, i)

        each_place(stages)
        return 0

    lax.fori_loop(0, chunks + max(DELIVER_LAG.values()), step, 0)

    for j in range(chunks - PAIR_OUT, chunks):
        pair_copy(j).wait_send()

    def flush(d):
        for j in range(chunks - KEEP[d], chunks):
            finish(d, j)
        if d != 1:
            for j in range(chunks - PART, chunks):
                for q in range(PIECES):
                    part_copy(j, q, from_a, a_rsem, FROM_A, down).wait_send()

    each_place(flush)
    for n in range(matrices):
        theirs = out_hbm.at[n, pl.ds(pl.multiple_of((1 - core) * half, 16), half), :]
        remote(theirs, theirs, out_rsem.at[n], out_rsem.at[n], partner).wait_recv()


def sums(a, g, width=256):
    a, g = a[0], g[0]
    matrices, tokens, rows = a.shape
    columns = g.shape[2]
    half = rows // 2
    bf16 = jnp.bfloat16
    dma = pltpu.SemaphoreType.DMA
    return pl.pallas_call(
        functools.partial(kernel, width),
        out_shape=jax.ShapeDtypeStruct((matrices, rows, columns), bf16),
        in_specs=[pl.BlockSpec(memory_space=pl.ANY)] * 2,
        out_specs=pl.BlockSpec(memory_space=pl.ANY),
        scratch_shapes=[
            pltpu.VMEM((2, tokens, rows), bf16),
            pltpu.VMEM((2, tokens, width), bf16),
            pltpu.VMEM((OWN, rows, width), jnp.float32),
            pltpu.VMEM((PAIR_OUT, half, width), bf16),
            pltpu.VMEM((PAIR_IN, half, width), bf16),
            pltpu.VMEM((FROM_A, half, width), bf16),
            pltpu.VMEM((FROM_B, half, width), bf16),
            pltpu.VMEM((PART, half, width), bf16),
            pltpu.VMEM((RES, half, width), bf16),
            dma((2, SLICES)),
            dma((2,)),
            dma((PAIR_OUT,)),
            dma((PAIR_IN,)),
            dma((FROM_A, PIECES)),
            dma((FROM_B, PIECES)),
            dma((PART, PIECES)),
            dma((RES, PIECES)),
            dma((RES, PIECES)),
            dma((RES, PIECES)),
            dma((RES, PIECES)),
            dma((RES, PIECES)),
            dma((matrices,)),
        ],
        compiler_params=pltpu.CompilerParams(collective_id=0, has_side_effects=True, vmem_limit_bytes=67043328),
        name="grad_sums",
    )(a, g)


def solution(mesh):
    P = jax.sharding.PartitionSpec
    return jax.shard_map(
        sums, mesh=mesh, in_specs=(P(("rep", "dp")), P(("rep", "dp"))), out_specs=P("rep"), check_vma=False)
```

```python
import functools

import jax
import jax.numpy as jnp
from jax import lax
from jax.experimental import pallas as pl
from jax.experimental.pallas import tpu as pltpu

COMBINE_LAG = {0: 1, 1: 5, 2: 3, 3: 1}
DELIVER_LAG = {0: 7, 1: 5, 2: 7, 3: 10}
PAIR_OUT, PAIR_IN, FROM_A, FROM_B, PART, RES = 2, 12, 12, 8, 6, 16
OWN = max(COMBINE_LAG.values()) + 1
SLICES = 4
BF16 = jnp.bfloat16


def groups(rows):
    first = (rows // 2 + 127) // 128 * 128
    return (0, first, first // 2), (first, rows - first, (rows - first) // 2)


def kernel(width, a_hbm, g_hbm, out, a_buf, g_buf, own, pair_out, pair_in, from_a, from_b, part,
           a_sem, g_sem, pair_ssem, pair_rsem, a_rsem, b_rsem, part_ssem, res_rsem, up_sem, down_sem,
           swap_ssem, swap_rsem):
    matrices, tokens, rows = a_hbm.shape
    per = g_hbm.shape[2] // width
    chunks = matrices * per
    blocks = 2 * chunks
    half = rows // 2
    depth = tokens // SLICES
    group = groups(rows)

    me = lax.axis_index("dp")
    chip, core = me // 2, me % 2
    place = chip + core * (3 - 2 * chip)
    step_to = 2 - 4 * core
    partner = me + 1 - 2 * core
    up, down = me + step_to, me - step_to

    barrier = pltpu.get_barrier_semaphore()

    def hello(device):
        pl.semaphore_signal(barrier, inc=1, device_id={"dp": device}, device_id_type=pl.DeviceIdType.MESH)

    hello(partner)
    pl.when(place > 0)(lambda: hello(down))
    pl.when(place < 3)(lambda: hello(up))

    def a_load(n, h, k):
        window = (pl.ds(k * depth, depth), pl.ds(group[h][0], group[h][1]))
        return pltpu.make_async_copy(a_hbm.at[(n, *window)], a_buf.at[(n % 2, *window)], a_sem.at[n % 2, h, k])

    def g_load(s):
        return pltpu.make_async_copy(
            g_hbm.at[s // per, :, pl.ds(pl.multiple_of((s % per) * width, width), width)], g_buf.at[s % 2],
            g_sem.at[s % 2])

    for h in range(2):
        for k in range(SLICES):
            a_load(0, h, k).start()
            if h == k == 0:
                g_load(0).start()
    pl.semaphore_wait(barrier, 1 + (place > 0).astype(jnp.int32) + (place < 3).astype(jnp.int32))

    def remote(src, dst, ssem, rsem, device):
        return pltpu.make_async_remote_copy(
            src_ref=src, dst_ref=dst, send_sem=ssem, recv_sem=rsem, device_id={"dp": device},
            device_id_type=pl.DeviceIdType.MESH)

    def pair_copy(b, h):
        r = pl.ds(0, group[h][2])
        return remote(pair_out.at[b % PAIR_OUT, r], pair_in.at[b % PAIR_IN, r], pair_ssem.at[b % PAIR_OUT],
                      pair_rsem.at[b % PAIR_IN], partner)

    def part_copy(b, h, box, rsem, slots, device):
        r = pl.ds(0, group[h][2])
        return remote(part.at[b % PART, r], box.at[b % slots, r], part_ssem.at[b % PART], rsem.at[b % slots], device)

    def to_a(b, h, device):
        return part_copy(b, h, from_a, a_rsem, FROM_A, device)

    def to_b(b, h, device):
        return part_copy(b, h, from_b, b_rsem, FROM_B, device)

    def spot(b, h):
        s = b // 2
        first, _, share = group[h]
        return out.at[s // per, pl.ds(pl.multiple_of(first + core * share, 16), share),
                      pl.ds(pl.multiple_of((s % per) * width, width), width)]

    def res_copy(b, h, ssem, device):
        return remote(spot(b, h), spot(b, h), ssem.at[b // 2 // per], res_rsem.at[b % RES], device)

    def swap_copy(b, h):
        n = b // 2 // per
        return remote(spot(b, h), spot(b, h), swap_ssem.at[n], swap_rsem.at[n], partner)

    def combine(d, b, h):
        pair_copy(b, h).wait_recv()
        r = pl.ds(0, group[h][2])
        if d == 2:
            to_a(b, h, up).wait_recv()
        if d == 1:
            to_a(b, h, down).wait_recv()
            to_b(b, h, up).wait_recv()
        total = own[b % OWN, r, :] + pair_in[b % PAIR_IN, r, :].astype(jnp.float32)
        if d in (1, 2):
            total += from_a[b % FROM_A, r, :].astype(jnp.float32)
        if d == 1:
            total += from_b[b % FROM_B, r, :].astype(jnp.float32)
            spot(b, h)[...] = total.astype(BF16)
            res_copy(b, h, up_sem, up).start()
            res_copy(b, h, down_sem, down).start()
            swap_copy(b, h).start()
            return
        copy = functools.partial(to_b if d == 2 else to_a, h=h, device=up if d == 0 else down)
        pl.when(b >= PART)(lambda: copy(b - PART).wait_send())
        part[b % PART, r, :] = total.astype(BF16)
        copy(b).start()

    def deliver(d, b, h):
        res_copy(b, h, up_sem, up).wait_recv()
        if d == 2:
            res_copy(b, h, up_sem, up).start()
        swap_copy(b, h).start()

    def each_place(f):
        for d in range(4):
            pl.when(place == d)(functools.partial(f, d))

    def guarded(b, f, *args):
        pl.when((b >= 0) & (b < blocks))(functools.partial(f, *args))

    def step(s, _):
        n, t = s // per, s % per
        for h in range(2):
            b = 2 * s + h

            @pl.when(s < chunks)
            def _():
                if h == 0:
                    pl.when(s + 1 < chunks)(lambda: g_load(s + 1).start())

                @pl.when((n + 1 < matrices) & (t < SLICES))
                def _():
                    a_load(n + 1, h, t).start()

                @pl.when(t == 0)
                def _():
                    for k in range(SLICES):
                        a_load(n, h, k).wait()

                if h == 0:
                    g_load(s).wait()
                first, count, share = group[h]
                r = pl.ds(0, share)
                term = lax.dot_general(
                    a_buf[n % 2, :, first:first + count], g_buf[s % 2], (((0,), (0,)), ((), ())),
                    preferred_element_type=jnp.float32)
                pl.when(b >= PAIR_OUT)(lambda: pair_copy(b - PAIR_OUT, h).wait_send())
                own[b % OWN, r, :] = jnp.where(core == 0, term[:share], term[share:])
                pair_out[b % PAIR_OUT, r, :] = jnp.where(core == 0, term[share:], term[:share]).astype(BF16)
                pair_copy(b, h).start()

            def stages(d):
                j = b - COMBINE_LAG[d]
                guarded(j, combine, d, j, (h - COMBINE_LAG[d]) % 2)
                if d != 1:
                    i = b - DELIVER_LAG[d]
                    guarded(i, deliver, d, i, (h - DELIVER_LAG[d]) % 2)

            each_place(stages)
        return 0

    lax.fori_loop(0, chunks + (max(DELIVER_LAG.values()) + 1) // 2, step, 0)

    for b in range(blocks - PAIR_OUT, blocks):
        pair_copy(b, b % 2).wait_send()

    def flush(d):
        if d != 1:
            for b in range(blocks - PART, blocks):
                to_a(b, b % 2, down).wait_send()
        for n in range(matrices):
            share = out.at[n, pl.ds(0, half), :]
            if d in (1, 2):
                remote(share, share, up_sem.at[n], swap_rsem.at[n], up).wait_send()
            if d == 1:
                remote(share, share, down_sem.at[n], swap_rsem.at[n], down).wait_send()
            swap = remote(share, share, swap_ssem.at[n], swap_rsem.at[n], partner)
            swap.wait_send()
            swap.wait_recv()

    each_place(flush)


def write(sums_ref, out_ref, sem):
    copies = [pltpu.make_async_copy(sums_ref.at[n], out_ref.at[n], sem.at[n]) for n in range(sums_ref.shape[0])]
    for c in copies:
        c.start()
    for c in copies:
        c.wait()


def sums(a, g, width=256):
    a, g = a[0], g[0]
    matrices, tokens, rows = a.shape
    shape = (matrices, rows, g.shape[2])
    share = groups(rows)[0][2]
    dma = pltpu.SemaphoreType.DMA
    anywhere, vmem = pl.BlockSpec(memory_space=pl.ANY), pl.BlockSpec(memory_space=pltpu.VMEM)
    held = pl.pallas_call(
        functools.partial(kernel, width),
        out_shape=pltpu.VMEM(shape, BF16),
        in_specs=[anywhere] * 2,
        out_specs=vmem,
        scratch_shapes=[
            pltpu.VMEM((2, tokens, rows), BF16),
            pltpu.VMEM((2, tokens, width), BF16),
            pltpu.VMEM((OWN, share, width), jnp.float32),
            pltpu.VMEM((PAIR_OUT, share, width), BF16),
            pltpu.VMEM((PAIR_IN, share, width), BF16),
            pltpu.VMEM((FROM_A, share, width), BF16),
            pltpu.VMEM((FROM_B, share, width), BF16),
            pltpu.VMEM((PART, share, width), BF16),
            dma((2, 2, SLICES)),
            dma((2,)),
            dma((PAIR_OUT,)),
            dma((PAIR_IN,)),
            dma((FROM_A,)),
            dma((FROM_B,)),
            dma((PART,)),
            dma((RES,)),
            dma((matrices,)),
            dma((matrices,)),
            dma((matrices,)),
            dma((matrices,)),
        ],
        compiler_params=pltpu.CompilerParams(collective_id=0, has_side_effects=True, vmem_limit_bytes=48_600_000),
        name="grad_sums",
    )(a, g)
    return pl.pallas_call(
        write,
        out_shape=jax.ShapeDtypeStruct(shape, BF16),
        in_specs=[vmem],
        out_specs=anywhere,
        scratch_shapes=[dma((matrices,))],
        compiler_params=pltpu.CompilerParams(vmem_limit_bytes=1 << 20),
        name="write_sums",
    )(held)


def solution(mesh):
    P = jax.sharding.PartitionSpec
    return jax.shard_map(
        sums, mesh=mesh, in_specs=(P(("rep", "dp")), P(("rep", "dp"))), out_specs=P("rep"), check_vma=False)
```

```python
import functools

import jax
import jax.numpy as jnp
from jax import lax
from jax.experimental import pallas as pl
from jax.experimental.pallas import tpu as pltpu

COMBINE_LAG = {1: 5, 2: 3, 3: 1}
DELIVER_LAG = {0: 10, 1: 8, 2: 6}
PAIR_OUT, PAIR_IN, FROM_A, FROM_B, PART, RES = 4, 24, 12, 12, 8, 16
OWN = 6
SLICES = 4
BF16 = jnp.bfloat16


def groups(rows):
    first = (rows // 2 + 127) // 128 * 128
    return (0, first, first // 2), (first, rows - first, (rows - first) // 2)


def kernel(width, a_hbm, g_hbm, out, a_buf, g_buf, own, pair_out, pair_in, from_a, from_b, part, held,
           a_sem, g_sem, pair_ssem, pair_rsem, a_rsem, b_rsem, part_ssem, res_rsem, down_sem, swap_ssem, swap_rsem):
    matrices, tokens, rows = a_hbm.shape
    per = g_hbm.shape[2] // width
    chunks = matrices * per
    blocks = 2 * chunks
    half = rows // 2
    depth = tokens // SLICES
    group = groups(rows)

    me = lax.axis_index("dp")
    chip, core = me // 2, me % 2
    place = 3 - chip + core * (2 * chip - 3)
    partner = me + 1 - 2 * core
    down, up = me + 2 - 4 * core, me - 2 + 4 * core
    beside = down + 1 - 2 * core

    barrier = pltpu.get_barrier_semaphore()

    def hello(device):
        pl.semaphore_signal(barrier, inc=1, device_id={"dp": device}, device_id_type=pl.DeviceIdType.MESH)

    hello(partner)
    pl.when(place > 0)(lambda: hello(down))
    pl.when(place < 3)(lambda: hello(up))
    pl.when(place == 3)(lambda: hello(beside))
    pl.when(place == 1)(lambda: hello(down + 1 - 2 * core))

    def a_load(n, h, k):
        window = (pl.ds(k * depth, depth), pl.ds(group[h][0], group[h][1]))
        return pltpu.make_async_copy(a_hbm.at[(n, *window)], a_buf.at[(n % 2, *window)], a_sem.at[n % 2, h, k])

    def g_load(s):
        return pltpu.make_async_copy(
            g_hbm.at[s // per, :, pl.ds(pl.multiple_of((s % per) * width, width), width)], g_buf.at[s % 2],
            g_sem.at[s % 2])

    g_load(0).start()
    for k in range(SLICES):
        a_load(0, 0, k).start()
    pl.semaphore_wait(barrier, jnp.where((place == 1) | (place == 3), 3 + (place == 1).astype(jnp.int32),
                                         2 + (place == 2).astype(jnp.int32)))

    def remote(src, dst, ssem, rsem, device):
        return pltpu.make_async_remote_copy(
            src_ref=src, dst_ref=dst, send_sem=ssem, recv_sem=rsem, device_id={"dp": device},
            device_id_type=pl.DeviceIdType.MESH)

    def pair_copy(i, h):
        r = pl.ds(0, group[h][2])
        return remote(pair_out.at[i % PAIR_OUT, r], pair_in.at[i % PAIR_IN, r], pair_ssem.at[i % PAIR_OUT],
                      pair_rsem.at[i % PAIR_IN], partner)

    def to_a(i, b, h, device):
        r = pl.ds(0, group[h][2])
        return remote(part.at[i % PART, r], from_a.at[b % FROM_A, r], part_ssem.at[i % PART], a_rsem.at[b % FROM_A],
                      device)

    def to_b(b, h):
        r = pl.ds(0, group[h][2])
        return remote(part.at[b % PART, r], from_b.at[b % FROM_B, r], part_ssem.at[b % PART], b_rsem.at[b % FROM_B],
                      down)

    def spot(b, h, c):
        s = b // 2
        first, _, share = group[h]
        whose = core if c == 0 else 1 - core
        return out.at[s // per, pl.ds(pl.multiple_of(first + whose * share, 16), share),
                      pl.ds(pl.multiple_of((s % per) * width, width), width)]

    def down_copy(b, h, c):
        return remote(spot(b, h, c), spot(b, h, c), down_sem.at[b // 2 // per, c], res_rsem.at[c, b % RES], down)

    def swap_copy(b, h, c, onward=False):
        n = b // 2 // per
        return remote(spot(b, h, c), spot(b, h, c), swap_ssem.at[n, c],
                      res_rsem.at[1, b % RES] if onward else swap_rsem.at[n, c], partner)

    def multiplied(d, b, h):
        share = group[h][2]
        r = pl.ds(0, share)
        mine = held[pl.ds(pl.multiple_of(core * share, 16), share), :]
        other = held[pl.ds(pl.multiple_of((1 - core) * share, 16), share), :]
        if d == 3:
            own[(2 * b) % OWN, r, :] = mine
            own[(2 * b + 1) % OWN, r, :] = other
            return
        if d == 0:
            for c, value in enumerate((other, mine)):
                i = 2 * b + c
                pl.when(i >= PAIR_OUT)(lambda: pair_copy(i - PAIR_OUT, (h - PAIR_OUT // 2) % 2).wait_send())
                pair_out[i % PAIR_OUT, r, :] = value.astype(BF16)
            for c in range(2):
                pair_copy(2 * b + c, h).start()
            return
        own[b % OWN, r, :] = mine
        pl.when(b >= PAIR_OUT)(lambda: pair_copy(b - PAIR_OUT, h).wait_send())
        pair_out[b % PAIR_OUT, r, :] = other.astype(BF16)
        pair_copy(b, h).start()

    def combine(d, b, h):
        r = pl.ds(0, group[h][2])

        def local(i):
            return own[i % OWN, r, :] + pair_in[i % PAIR_IN, r, :].astype(jnp.float32)

        if d == 3:
            for c, device in enumerate((down, beside)):
                i = 2 * b + c
                pair_copy(i, h).wait_recv()
                total = local(i)
                pl.when(i >= PART)(lambda: to_a(i - PART, b, (h - PART // 2) % 2, device).wait_send())
                part[i % PART, r, :] = total.astype(BF16)
                to_a(i, b, h, device).start()
            return
        pair_copy(b, h).wait_recv()
        to_a(b, b, h, up).wait_recv()
        if d == 1:
            to_b(b, h).wait_recv()
        total = local(b) + from_a[b % FROM_A, r, :].astype(jnp.float32)
        if d == 2:
            pl.when(b >= PART)(lambda: to_b(b - PART, h).wait_send())
            part[b % PART, r, :] = total.astype(BF16)
            to_b(b, h).start()
            return
        total += from_b[b % FROM_B, r, :].astype(jnp.float32)
        spot(b, h, 0)[...] = total.astype(BF16)
        down_copy(b, h, 0).start()
        swap_copy(b, h, 0, onward=True).start()

    def deliver(d, b, h):
        if d == 0:
            down_copy(b, h, 0).wait_recv()
            swap_copy(b, h, 0).start()
        down_copy(b, h, 1).wait_recv()
        if d != 0:
            down_copy(b, h, 1).start()
        if d != 2:
            swap_copy(b, h, 1).start()

    def each_place(f):
        for d in range(4):
            pl.when(place == d)(functools.partial(f, d))

    def guarded(b, f, *args):
        pl.when((b >= 0) & (b < blocks))(functools.partial(f, *args))

    def step(s, _):
        n, t = s // per, s % per
        for h in range(2):
            b = 2 * s + h

            @pl.when(s < chunks)
            def _():
                @pl.when(t == 0)
                def _():
                    for k in range(SLICES):
                        a_load(n, h, k).wait()

                if h == 0:
                    g_load(s).wait()

                    @pl.when(s == 0)
                    def _():
                        for k in range(SLICES):
                            a_load(0, 1, k).start()

                pl.when((s + 1 < chunks) & ((s == 0) if h else (s > 0)))(lambda: g_load(s + 1).start())

                @pl.when((n + 1 < matrices) & (t >= 1) & (t <= SLICES))
                def _():
                    a_load(n + 1, h, t - 1).start()

                first, count, _ = group[h]
                held[:count] = lax.dot_general(
                    a_buf[n % 2, :, first:first + count], g_buf[s % 2], (((0,), (0,)), ((), ())),
                    preferred_element_type=jnp.float32)
                each_place(lambda d: multiplied(d, b, h))

            def stages(d):
                if d != 0:
                    j = b - COMBINE_LAG[d]
                    guarded(j, combine, d, j, (h - COMBINE_LAG[d]) % 2)
                if d != 3:
                    i = b - DELIVER_LAG[d]
                    guarded(i, deliver, d, i, (h - DELIVER_LAG[d]) % 2)

            each_place(stages)
        return 0

    lax.fori_loop(0, chunks + (max(DELIVER_LAG.values()) + 1) // 2, step, 0)

    def flush(d):
        if d in (1, 2):
            for b in range(blocks - PAIR_OUT, blocks):
                pair_copy(b, b % 2).wait_send()
        if d == 0:
            for i in range(2 * blocks - PAIR_OUT, 2 * blocks):
                pair_copy(i, i // 2 % 2).wait_send()
        if d == 2:
            for b in range(blocks - PART, blocks):
                to_b(b, b % 2).wait_send()
        if d == 3:
            for i in range(2 * blocks - PART, 2 * blocks):
                to_a(i, i // 2, i // 2 % 2, down).wait_send()
        for n in range(matrices):
            share = out.at[n, pl.ds(0, half), :]
            for c in range(2):
                if d == 1 or (d == 2 and c == 1):
                    remote(share, share, down_sem.at[n, c], swap_rsem.at[n, c], down).wait_send()
                if d in (0, 1):
                    remote(share, share, swap_ssem.at[n, c], swap_rsem.at[n, c], partner).wait_send()
                if d == 3 or (d == 2 and c == 1):
                    remote(share, share, swap_ssem.at[n, c], swap_rsem.at[n, c], partner).wait_recv()

    each_place(flush)


def write(sums_ref, out_ref, sem):
    parts = sem.shape[1]
    rows = sums_ref.shape[1] // parts
    copies = [
        pltpu.make_async_copy(sums_ref.at[n, pl.ds(k * rows, rows), :], out_ref.at[n, pl.ds(k * rows, rows), :],
                              sem.at[n, k])
        for n in range(sums_ref.shape[0]) for k in range(parts)]
    for c in copies:
        c.start()
    for c in copies:
        c.wait()


def sums(a, g, width=256):
    a, g = a[0], g[0]
    matrices, tokens, rows = a.shape
    shape = (matrices, rows, g.shape[2])
    share = groups(rows)[0][2]
    dma = pltpu.SemaphoreType.DMA
    anywhere, vmem = pl.BlockSpec(memory_space=pl.ANY), pl.BlockSpec(memory_space=pltpu.VMEM)
    total = pl.pallas_call(
        functools.partial(kernel, width),
        out_shape=pltpu.VMEM(shape, BF16),
        in_specs=[anywhere] * 2,
        out_specs=vmem,
        scratch_shapes=[
            pltpu.VMEM((2, tokens, rows), BF16),
            pltpu.VMEM((2, tokens, width), BF16),
            pltpu.VMEM((OWN, share, width), jnp.float32),
            pltpu.VMEM((PAIR_OUT, share, width), BF16),
            pltpu.VMEM((PAIR_IN, share, width), BF16),
            pltpu.VMEM((FROM_A, share, width), BF16),
            pltpu.VMEM((FROM_B, share, width), BF16),
            pltpu.VMEM((PART, share, width), BF16),
            pltpu.VMEM((2 * share, width), jnp.float32),
            dma((2, 2, SLICES)),
            dma((2,)),
            dma((PAIR_OUT,)),
            dma((PAIR_IN,)),
            dma((FROM_A,)),
            dma((FROM_B,)),
            dma((PART,)),
            dma((2, RES)),
            dma((matrices, 2)),
            dma((matrices, 2)),
            dma((matrices, 2)),
        ],
        compiler_params=pltpu.CompilerParams(collective_id=0, has_side_effects=True, vmem_limit_bytes=48_600_000),
        name="grad_sums",
    )(a, g)
    return pl.pallas_call(
        write,
        out_shape=jax.ShapeDtypeStruct(shape, BF16),
        in_specs=[vmem],
        out_specs=anywhere,
        scratch_shapes=[dma((matrices, 4))],
        compiler_params=pltpu.CompilerParams(vmem_limit_bytes=1 << 20),
        name="write_sums",
    )(total)


def solution(mesh):
    P = jax.sharding.PartitionSpec
    return jax.shard_map(
        sums, mesh=mesh, in_specs=(P(("rep", "dp")), P(("rep", "dp"))), out_specs=P("rep"), check_vma=False)
```

```python
import functools

import jax
import jax.numpy as jnp
from jax import lax
from jax.experimental import pallas as pl
from jax.experimental.pallas import tpu as pltpu

COMBINE_LAG = {1: 3, 2: 1, 3: 0}
DELIVER_LAG = {0: 11, 1: 6, 2: 3}
PAIR_OUT, PAIR_IN, FROM_A, FROM_B, PART, RES = 4, 24, 12, 12, 8, 16
OWN = 6
SLICES = 4
BF16 = jnp.bfloat16


def groups(rows):
    first = (rows // 2 + 127) // 128 * 128
    return (0, first, first // 2), (first, rows - first, (rows - first) // 2)


def kernel(width, a_hbm, g_hbm, out, a_buf, g_buf, own, pair_out, pair_in, from_a, from_b, part, held,
           a_sem, g_sem, pair_ssem, pair_rsem, a_rsem, b_rsem, part_ssem, res_rsem, down_sem, swap_ssem, swap_rsem):
    matrices, tokens, rows = a_hbm.shape
    per = g_hbm.shape[2] // width
    chunks = matrices * per
    blocks = 2 * chunks
    half = rows // 2
    depth = tokens // SLICES
    group = groups(rows)

    me = lax.axis_index("dp")
    chip, core = me // 2, me % 2
    place = 3 - chip + core * (2 * chip - 3)
    partner = me + 1 - 2 * core
    down, up = me + 2 - 4 * core, me - 2 + 4 * core
    beside = down + 1 - 2 * core

    barrier = pltpu.get_barrier_semaphore()

    def hello(device):
        pl.semaphore_signal(barrier, inc=1, device_id={"dp": device}, device_id_type=pl.DeviceIdType.MESH)

    def a_load(n, h, k):
        window = (pl.ds(k * depth, depth), pl.ds(group[h][0], group[h][1]))
        return pltpu.make_async_copy(a_hbm.at[(n, *window)], a_buf.at[(n % 2, *window)], a_sem.at[n % 2, h, k])

    def g_load(s):
        return pltpu.make_async_copy(
            g_hbm.at[s // per, :, pl.ds(pl.multiple_of((s % per) * width, width), width)], g_buf.at[s % 2],
            g_sem.at[s % 2, 0])

    def g_slice(k):
        window = pl.ds(k * depth, depth)
        return pltpu.make_async_copy(g_hbm.at[0, window, pl.ds(0, width)], g_buf.at[0, window], g_sem.at[0, k])

    for k in range(SLICES):
        g_slice(k).start()
        a_load(0, 0, k).start()

    hello(partner)
    pl.when(place > 0)(lambda: hello(down))
    pl.when(place < 3)(lambda: hello(up))
    pl.when(place == 3)(lambda: hello(beside))
    pl.when(place == 1)(lambda: hello(down + 1 - 2 * core))
    pl.semaphore_wait(barrier, jnp.where((place == 1) | (place == 3), 3 + (place == 1).astype(jnp.int32),
                                         2 + (place == 2).astype(jnp.int32)))

    def remote(src, dst, ssem, rsem, device):
        return pltpu.make_async_remote_copy(
            src_ref=src, dst_ref=dst, send_sem=ssem, recv_sem=rsem, device_id={"dp": device},
            device_id_type=pl.DeviceIdType.MESH)

    def pair_copy(i, h):
        r = pl.ds(0, group[h][2])
        return remote(pair_out.at[i % PAIR_OUT, r], pair_in.at[i % PAIR_IN, r], pair_ssem.at[i % PAIR_OUT],
                      pair_rsem.at[i % PAIR_IN], partner)

    def to_a(i, b, h, device):
        r = pl.ds(0, group[h][2])
        return remote(part.at[i % PART, r], from_a.at[b % FROM_A, r], part_ssem.at[i % PART], a_rsem.at[b % FROM_A],
                      device)

    def to_b(b, h):
        r = pl.ds(0, group[h][2])
        return remote(part.at[b % PART, r], from_b.at[b % FROM_B, r], part_ssem.at[b % PART], b_rsem.at[b % FROM_B],
                      down)

    def spot(b, h, c):
        s = b // 2
        first, _, share = group[h]
        whose = core if c == 0 else 1 - core
        return out.at[s // per, pl.ds(pl.multiple_of(first + whose * share, 16), share),
                      pl.ds(pl.multiple_of((s % per) * width, width), width)]

    def down_copy(b, h, c):
        return remote(spot(b, h, c), spot(b, h, c), down_sem.at[b // 2 // per, c], res_rsem.at[c, b % RES], down)

    def swap_copy(b, h, c, onward=False):
        n = b // 2 // per
        return remote(spot(b, h, c), spot(b, h, c), swap_ssem.at[n, c],
                      res_rsem.at[1, b % RES] if onward else swap_rsem.at[n, c], partner)

    def multiplied(d, b, h):
        share = group[h][2]
        r = pl.ds(0, share)
        mine = held[pl.ds(pl.multiple_of(core * share, 16), share), :]
        other = held[pl.ds(pl.multiple_of((1 - core) * share, 16), share), :]
        if d == 3:
            own[(2 * b) % OWN, r, :] = mine
            own[(2 * b + 1) % OWN, r, :] = other
            return
        if d == 0:
            for c, value in enumerate((other, mine)):
                i = 2 * b + c
                pl.when(i >= PAIR_OUT)(lambda: pair_copy(i - PAIR_OUT, (h - PAIR_OUT // 2) % 2).wait_send())
                pair_out[i % PAIR_OUT, r, :] = value.astype(BF16)
            for c in range(2):
                pair_copy(2 * b + c, h).start()
            return
        own[b % OWN, r, :] = mine
        pl.when(b >= PAIR_OUT)(lambda: pair_copy(b - PAIR_OUT, h).wait_send())
        pair_out[b % PAIR_OUT, r, :] = other.astype(BF16)
        pair_copy(b, h).start()

    def combine(d, b, h):
        r = pl.ds(0, group[h][2])

        def local(i):
            return own[i % OWN, r, :] + pair_in[i % PAIR_IN, r, :].astype(jnp.float32)

        if d == 3:
            for c, device in enumerate((down, beside)):
                i = 2 * b + c
                pair_copy(i, h).wait_recv()
                total = local(i)
                pl.when(i >= PART)(lambda: to_a(i - PART, b, (h - PART // 2) % 2, device).wait_send())
                part[i % PART, r, :] = total.astype(BF16)
                to_a(i, b, h, device).start()
            return
        pair_copy(b, h).wait_recv()
        to_a(b, b, h, up).wait_recv()
        if d == 1:
            to_b(b, h).wait_recv()
        total = local(b) + from_a[b % FROM_A, r, :].astype(jnp.float32)
        if d == 2:
            pl.when(b >= PART)(lambda: to_b(b - PART, h).wait_send())
            part[b % PART, r, :] = total.astype(BF16)
            to_b(b, h).start()
            return
        total += from_b[b % FROM_B, r, :].astype(jnp.float32)
        spot(b, h, 0)[...] = total.astype(BF16)
        down_copy(b, h, 0).start()
        swap_copy(b, h, 0, onward=True).start()

    def deliver(d, b, h):
        if d == 0:
            down_copy(b, h, 0).wait_recv()
            swap_copy(b, h, 0).start()
        down_copy(b, h, 1).wait_recv()
        if d != 0:
            down_copy(b, h, 1).start()
        if d != 2:
            swap_copy(b, h, 1).start()

    def each_place(f):
        for d in range(4):
            pl.when(place == d)(functools.partial(f, d))

    def guarded(b, f, *args):
        pl.when((b >= 0) & (b < blocks))(functools.partial(f, *args))

    def step(s, _):
        n, t = s // per, s % per
        for h in range(2):
            b = 2 * s + h

            @pl.when(s < chunks)
            def _():
                first, count, _ = group[h]

                def multiply():
                    @pl.when(t == 0)
                    def _():
                        for k in range(SLICES):
                            a_load(n, h, k).wait()

                    if h == 0:
                        g_load(s).wait()
                    pl.when((s + 1 < chunks) & ((s == 0) if h else (s > 0)))(lambda: g_load(s + 1).start())

                    @pl.when((n + 1 < matrices) & (t >= 1) & (t <= SLICES))
                    def _():
                        a_load(n + 1, h, t - 1).start()

                    held[:count] = lax.dot_general(
                        a_buf[n % 2, :, first:first + count], g_buf[s % 2], (((0,), (0,)), ((), ())),
                        preferred_element_type=jnp.float32)

                def chase():
                    for k in range(SLICES):
                        a_load(0, 0, k).wait()
                        g_slice(k).wait()
                        for later in {1: (0,), 2: (1,), 3: (2, 3)}.get(k, ()):
                            a_load(0, 1, later).start()
                        window = slice(k * depth, (k + 1) * depth)
                        term = lax.dot_general(
                            a_buf[0, window, :count], g_buf[0, window], (((0,), (0,)), ((), ())),
                            preferred_element_type=jnp.float32)
                        held[:count] = term if k == 0 else held[:count] + term

                if h == 0:
                    pl.when(s == 0)(chase)
                    pl.when(s > 0)(multiply)
                else:
                    multiply()
                each_place(lambda d: multiplied(d, b, h))

            def stages(d):
                if d != 0:
                    j = b - COMBINE_LAG[d]
                    guarded(j, combine, d, j, (h - COMBINE_LAG[d]) % 2)
                if d != 3:
                    i = b - DELIVER_LAG[d]
                    guarded(i, deliver, d, i, (h - DELIVER_LAG[d]) % 2)

            each_place(stages)
        return 0

    lax.fori_loop(0, chunks + (max(DELIVER_LAG.values()) + 1) // 2, step, 0)

    def flush(d):
        if d in (1, 2):
            for b in range(blocks - PAIR_OUT, blocks):
                pair_copy(b, b % 2).wait_send()
        if d == 0:
            for i in range(2 * blocks - PAIR_OUT, 2 * blocks):
                pair_copy(i, i // 2 % 2).wait_send()
        if d == 2:
            for b in range(blocks - PART, blocks):
                to_b(b, b % 2).wait_send()
        if d == 3:
            for i in range(2 * blocks - PART, 2 * blocks):
                to_a(i, i // 2, i // 2 % 2, down).wait_send()
        for n in range(matrices):
            share = out.at[n, pl.ds(0, half), :]
            for c in range(2):
                if d == 1 or (d == 2 and c == 1):
                    remote(share, share, down_sem.at[n, c], swap_rsem.at[n, c], down).wait_send()
                if d in (0, 1):
                    remote(share, share, swap_ssem.at[n, c], swap_rsem.at[n, c], partner).wait_send()
                if d == 3 or (d == 2 and c == 1):
                    remote(share, share, swap_ssem.at[n, c], swap_rsem.at[n, c], partner).wait_recv()

    each_place(flush)


def write(sums_ref, out_ref, sem):
    parts = sem.shape[1]
    rows = sums_ref.shape[1] // parts
    copies = [
        pltpu.make_async_copy(sums_ref.at[n, pl.ds(k * rows, rows), :], out_ref.at[n, pl.ds(k * rows, rows), :],
                              sem.at[n, k])
        for n in range(sums_ref.shape[0]) for k in range(parts)]
    for c in copies:
        c.start()
    for c in copies:
        c.wait()


def sums(a, g, width=256):
    a, g = a[0], g[0]
    matrices, tokens, rows = a.shape
    shape = (matrices, rows, g.shape[2])
    share = groups(rows)[0][2]
    dma = pltpu.SemaphoreType.DMA
    anywhere, vmem = pl.BlockSpec(memory_space=pl.ANY), pl.BlockSpec(memory_space=pltpu.VMEM)
    total = pl.pallas_call(
        functools.partial(kernel, width),
        out_shape=pltpu.VMEM(shape, BF16),
        in_specs=[anywhere] * 2,
        out_specs=vmem,
        scratch_shapes=[
            pltpu.VMEM((2, tokens, rows), BF16),
            pltpu.VMEM((2, tokens, width), BF16),
            pltpu.VMEM((OWN, share, width), jnp.float32),
            pltpu.VMEM((PAIR_OUT, share, width), BF16),
            pltpu.VMEM((PAIR_IN, share, width), BF16),
            pltpu.VMEM((FROM_A, share, width), BF16),
            pltpu.VMEM((FROM_B, share, width), BF16),
            pltpu.VMEM((PART, share, width), BF16),
            pltpu.VMEM((2 * share, width), jnp.float32),
            dma((2, 2, SLICES)),
            dma((2, SLICES)),
            dma((PAIR_OUT,)),
            dma((PAIR_IN,)),
            dma((FROM_A,)),
            dma((FROM_B,)),
            dma((PART,)),
            dma((2, RES)),
            dma((matrices, 2)),
            dma((matrices, 2)),
            dma((matrices, 2)),
        ],
        compiler_params=pltpu.CompilerParams(collective_id=0, has_side_effects=True, vmem_limit_bytes=48_600_000),
        name="grad_sums",
    )(a, g)
    return pl.pallas_call(
        write,
        out_shape=jax.ShapeDtypeStruct(shape, BF16),
        in_specs=[vmem],
        out_specs=anywhere,
        scratch_shapes=[dma((matrices, 4))],
        compiler_params=pltpu.CompilerParams(vmem_limit_bytes=1 << 20),
        name="write_sums",
    )(total)


def solution(mesh):
    P = jax.sharding.PartitionSpec
    return jax.shard_map(
        sums, mesh=mesh, in_specs=(P(("rep", "dp")), P(("rep", "dp"))), out_specs=P("rep"), check_vma=False)
```
